32 devices in a mesh: gx: 4 (over z), gy: 8 (over y, x, core).
Axes of the slice: x: 2, y: 2, z: 4, core: 2. Of those that a mesh axis runs over, the one named last changes fastest.
Arguments:
- x_gen: bfloat16 [8, 512, 3072], P('gy', 'gx'), may hold values from -6 to 6
- fresh_noise: bfloat16 [8, 512, 3072], P('gy', 'gx'), may hold values from -6 to 6
- steps_t: int32 [8], P('gy'), may hold values from 0 to 999
- real_mod: float32 [8, 2, 3072], P('gy'), may hold values from -2.5 to 2.5
- real_w_up: bfloat16 [3072, 6144], P(None, 'gx'), may hold values from -0.109375 to 0.109375
- real_b_up: float32 [6144], P('gx'), may hold values from -3 to 3
- real_w_down: bfloat16 [6144, 3072], P('gx'), may hold values from -0.078125 to 0.078125
- fake_mod: float32 [8, 2, 3072], P('gy'), may hold values from -2.5 to 2.5
- fake_w_up: bfloat16 [3072, 6144], P('gy', 'gx'), may hold values from -0.109375 to 0.109375
- fake_b_up: float32 [6144], P('gx'), may hold values from -3 to 3
- fake_w_down: bfloat16 [6144, 3072], P('gx', 'gy'), may hold values from -0.078125 to 0.078125
Outputs:
- dmd_grad: float32 [8, 512, 3072], P('gy', 'gx')
- fake_grad: float32 [3072, 6144], P('gy', 'gx')
The draws below stay inside these ranges and needn't reach their ends.
All inputs are finite; a program needn't handle non-finite values.
Results may differ from the reference program's by a relative error of at most 0.013.
Values may be sent and summed in bfloat16 or wider, within the bound.
A program may use at most 128 MiB of HBM per device.

```python
import jax
import jax.numpy as jnp
from jax import lax

D = 3072
FF = 6144
TSTEPS = 1000
SEQ = 512
SAMPLES = 8
N_GX = 4
N_GY = 8


def set_ends(entries, rng, smallest, high):
    spot = [jax.random.randint(jax.random.fold_in(rng, axis), (), 0, length) for axis, length in enumerate(entries.shape)]
    main_axis = entries.shape.index(max(entries.shape))
    neighbour = spot[:main_axis] + [(spot[main_axis] + 1) % entries.shape[main_axis]] + spot[main_axis + 1:]
    return entries.at[tuple(spot)].set(smallest).at[tuple(neighbour)].set(high)


def level_of(key, dims, cuts, least, top_value):
    def one(axis_at, blocks):
        draws = jax.random.uniform(jax.random.fold_in(jax.random.fold_in(key, 6), axis_at), (blocks,), jnp.float32, least / len(cuts), top_value / len(cuts))
        return jnp.repeat(jnp.exp(draws), dims[axis_at] // blocks).reshape((-1,) + (1,) * (len(dims) - axis_at - 1))

    factor_of = one(*cuts[0])
    for cut in cuts[1:]:
        factor_of = factor_of * one(*cut)
    return factor_of


def normal_values(own_key, dims, scale, reach, shards=(), dtype=jnp.bfloat16):
    array = jax.random.normal(own_key, dims, jnp.float32) * scale
    if len(shards) > 0:
        array = level_of(own_key, dims, shards, -0.22, 0.18) * array
    return jnp.clip(array, min=-reach, max=reach).astype(dtype)


def setup_inputs(seed: int = 0) -> dict:
    seeds = jax.random.split(jax.random.key(seed), 12)
    return {
        "x_gen": normal_values(seeds[0], (SAMPLES, SEQ, D), 1.0, 6.0, ((0, 8), (1, 4))),
        "fresh_noise": normal_values(seeds[1], (SAMPLES, SEQ, D), 1.0, 6.0, ((0, 8), (1, 4))),
        "steps_t": set_ends(jax.random.randint(seeds[2], (SAMPLES,), 0, TSTEPS), jax.random.fold_in(seeds[2], 1), 0, TSTEPS - 1).astype(jnp.int32),
        "real_mod": normal_values(seeds[3], (SAMPLES, 2, D), 0.3, 2.5, ((0, 8),), jnp.float32),
        "real_w_up": normal_values(seeds[4], (D, FF), D ** -0.5, 0.109375, ((1, 4),)),
        "real_b_up": normal_values(seeds[5], (FF,), 0.5, 3.0, ((0, 4),), jnp.float32),
        "real_w_down": normal_values(seeds[6], (FF, D), FF ** -0.5, 0.078125, ((0, 4),)),
        "fake_mod": normal_values(seeds[7], (SAMPLES, 2, D), 0.3, 2.5, ((0, 8),), jnp.float32),
        "fake_w_up": normal_values(seeds[8], (D, FF), D ** -0.5, 0.109375, ((0, 8), (1, 4))),
        "fake_b_up": normal_values(seeds[9], (FF,), 0.5, 3.0, ((0, 4),), jnp.float32),
        "fake_w_down": normal_values(seeds[10], (FF, D), FF ** -0.5, 0.078125, ((0, 4), (1, 8))),
    }


def layer_norm(values):
    center = values - lax.optimization_barrier(jnp.mean(values, axis=-1, keepdims=True))
    spread = lax.optimization_barrier(jnp.mean(center * center, axis=-1, keepdims=True))
    return center * lax.rsqrt(spread + 1e-06)

def net_pred(normed, modulation, w_up, b_up, w_down):
    modulated = (normed * (1.0 + modulation[1]) + modulation[0]).astype(jnp.bfloat16)
    hidden = jax.nn.gelu(jnp.dot(modulated, w_up, preferred_element_type=jnp.float32) + b_up, approximate=True).astype(jnp.bfloat16)
    group_size = FF // N_GX
    partials = jnp.einsum('sgk,gkd->gsd', hidden.reshape(SEQ, N_GX, group_size).astype(jnp.float32), w_down.reshape(N_GX, group_size, D).astype(jnp.float32))
    partials = lax.optimization_barrier(partials.astype(jnp.bfloat16)).astype(jnp.float32)
    return (lax.optimization_barrier(jnp.sum(partials, axis=0)), hidden)

def reference(x_gen, fresh_noise, steps_t, real_mod, real_w_up, real_b_up, real_w_down, fake_mod, fake_w_up, fake_b_up, fake_w_down):
    loss_scale = float(SEQ * N_GY) ** (-0.5)

    def per_sample(grad_total, inputs):
        clean, drawn, step_index, modulation_real, modulation_fake = inputs
        noise_level = (step_index.astype(jnp.float32) + 1.0) / TSTEPS
        clean_f = clean.astype(jnp.float32)
        drawn_f = drawn.astype(jnp.float32)
        noised = ((1.0 - noise_level) * clean_f + noise_level * drawn_f).astype(jnp.bfloat16)
        target = (drawn_f - clean_f).astype(jnp.bfloat16)
        normed = layer_norm(noised.astype(jnp.float32))
        pred_real, unused_hidden = net_pred(normed, modulation_real, real_w_up, real_b_up, real_w_down)
        pred_fake, hidden_fake = net_pred(normed, modulation_fake, fake_w_up, fake_b_up, fake_w_down)
        dmd_grad = pred_fake - pred_real
        error_v = (pred_fake - target.astype(jnp.float32)).astype(jnp.bfloat16)
        partial_term = jnp.dot(error_v.T, hidden_fake, preferred_element_type=jnp.float32) * loss_scale
        partial_term = lax.optimization_barrier(partial_term.astype(jnp.bfloat16)).astype(jnp.float32)
        return (grad_total + partial_term, dmd_grad)
    grad_start = jnp.zeros((D, FF), jnp.float32)
    fake_grad, dmd_grad = lax.scan(per_sample, grad_start, (x_gen, fresh_noise, steps_t, real_mod, fake_mod))
    return (dmd_grad, fake_grad)
```

```python
import jax
import jax.numpy as jnp
from jax import lax
from jax.sharding import PartitionSpec as P

TSTEPS = 1000
BF = jnp.bfloat16
F32 = jnp.float32


def layer_norm(values):
    center = values - jnp.mean(values, axis=-1, keepdims=True)
    spread = jnp.mean(center * center, axis=-1, keepdims=True)
    return center * lax.rsqrt(spread + 1e-06)


def halves(block):
    cut = block.shape[0] // 2
    return [block[:cut], block[cut:]]


def add(a, b):
    return a.astype(F32) + b.astype(F32)


def ring_shift(value, step):
    n = lax.axis_size("gx")
    return lax.ppermute(value, "gx", [(i, (i + step) % n) for i in range(n)])


def flip(value, bit):
    n = lax.axis_size("gy")
    return lax.ppermute(value, "gy", [(i, i ^ bit) for i in range(n)])


def ring_gather(own):
    n = lax.axis_size("gx")
    blocks = {0: own}
    if n == 1:
        return blocks
    far = n // 2
    for d in range(1, far):
        blocks[n - d] = ring_shift(blocks[(n - d + 1) % n], 1)
        blocks[d] = ring_shift(blocks[d - 1], -1)
    first = ring_shift(halves(blocks[(n - far + 1) % n])[0], 1)
    second = ring_shift(halves(blocks[far - 1])[1], -1)
    blocks[far] = jnp.concatenate([first, second], axis=0)
    return blocks


def ring_scatter(parts):
    n = lax.axis_size("gx")
    cut = [halves(part) for part in parts]
    total = [half.astype(F32) for half in cut[0]]
    far = n // 2
    for half in (0, 1):
        for step in (1, -1):
            start = far if (half == 0) == (step == 1) else far - 1
            if start < 1:
                continue
            running = cut[(step * start) % n][half]
            for d in range(start, 0, -1):
                got = ring_shift(running, step)
                if d > 1:
                    running = add(cut[(step * (d - 1)) % n][half], got).astype(BF)
                else:
                    total[half] = total[half] + got.astype(F32)
    return jnp.concatenate(total, axis=0)


def route(k):
    return k & -k, 1 << (k.bit_length() - 1)


def chip_offsets(n):
    return sorted(range(2, n, 2), key=lambda k: (bin(k).count("1"), k))


def plane_gather(own):
    n = lax.axis_size("gy")
    blocks = {0: own}
    for k in chip_offsets(n):
        low, high = route(k)
        if low == high:
            blocks[k] = flip(own, k)
        else:
            first = flip(halves(blocks[k ^ low])[0], low)
            second = flip(halves(blocks[k ^ high])[1], high)
            blocks[k] = jnp.concatenate([first, second], axis=0)
    for k in range(0, n, 2):
        blocks[k + 1] = flip(blocks[k], 1)
    return blocks


def plane_scatter(parts):
    n = lax.axis_size("gy")
    held = {k: halves(add(parts[k], flip(parts[k + 1], 1))) for k in range(0, n, 2)}
    for k in reversed(chip_offsets(n)):
        low, high = route(k)
        for half, bit in ((0, low), (1, high)):
            got = flip(held[k][half].astype(BF), bit)
            held[k ^ bit][half] = held[k ^ bit][half] + got.astype(F32)
    return jnp.concatenate(held[0], axis=0)


def shards(
    x_gen,
    fresh_noise,
    steps_t,
    real_mod,
    real_w_up,
    real_b_up,
    real_w_down,
    fake_mod,
    fake_w_up,
    fake_b_up,
    fake_w_down,
):
    n_gx, n_gy = lax.axis_size("gx"), lax.axis_size("gy")
    me = lax.axis_index("gy")
    noise_level = (steps_t[0].astype(F32) + 1.0) / TSTEPS
    clean_f = x_gen[0].astype(F32)
    drawn_f = fresh_noise[0].astype(F32)
    noised = ((1.0 - noise_level) * clean_f + noise_level * drawn_f).astype(BF)
    target = (drawn_f - clean_f).astype(BF)
    own_rows, width = noised.shape
    wide = fake_w_up.shape[0]

    up_blocks = plane_gather(fake_w_up)
    tokens = ring_gather(noised)
    down_blocks = plane_gather(fake_w_down)

    def columns(array, k):
        return lax.dynamic_slice_in_dim(array, (me ^ k) * wide, wide, axis=1)

    noised_all = jnp.concatenate([tokens[j] for j in range(n_gx)], axis=0)
    normed = layer_norm(noised_all.astype(F32))
    real_in = (normed * (1.0 + real_mod[0, 1]) + real_mod[0, 0]).astype(BF)
    fake_in = (normed * (1.0 + fake_mod[0, 1]) + fake_mod[0, 0]).astype(BF)
    real_in, fake_in = lax.optimization_barrier((real_in, fake_in))
    real_hidden = jax.nn.gelu(
        jnp.dot(real_in, real_w_up, preferred_element_type=F32) + real_b_up, approximate=True
    ).astype(BF)
    real_part = jnp.dot(real_hidden, real_w_down, preferred_element_type=F32).astype(BF)
    real_rows = ring_scatter([real_part[j * own_rows:(j + 1) * own_rows] for j in range(n_gx)])

    fake_pre = fake_b_up[None]
    for k in range(n_gy):
        fake_pre = fake_pre + jnp.dot(
            columns(fake_in, k), up_blocks[k], preferred_element_type=F32
        )
    fake_hidden = jax.nn.gelu(fake_pre, approximate=True).astype(BF)

    loss_scale = float(n_gy * n_gx * own_rows) ** (-0.5)
    dmd_grad = jnp.zeros((own_rows, width), F32)
    products = {}
    for k in range(0, n_gy, 2):
        pair = jnp.concatenate(
            [
                jnp.dot(fake_hidden, down_blocks[i], preferred_element_type=F32).astype(BF)
                for i in (k, k + 1)
            ],
            axis=1,
        )
        pred = ring_scatter([pair[j * own_rows:(j + 1) * own_rows] for j in range(n_gx)])
        goal = jnp.concatenate([columns(target, i) for i in (k, k + 1)], axis=1)
        error = ring_gather((pred - goal.astype(F32)).astype(BF))
        error_all = jnp.concatenate([error[j] for j in range(n_gx)], axis=0)
        for i in (0, 1):
            part = slice(i * wide, (i + 1) * wide)
            dmd_grad = lax.dynamic_update_slice_in_dim(
                dmd_grad, pred[:, part], (me ^ (k + i)) * wide, axis=1
            )
            product = lax.dot_general(
                error_all[:, part],
                fake_hidden,
                (((0,), (0,)), ((), ())),
                preferred_element_type=F32,
            )
            products[k + i] = (product * loss_scale).astype(BF)
    fake_grad = plane_scatter(products)
    return ((dmd_grad - real_rows)[None], fake_grad)


def solution(mesh):
    return jax.shard_map(
        shards,
        mesh=mesh,
        in_specs=(
            P("gy", "gx", None),
            P("gy", "gx", None),
            P("gy"),
            P("gy", None, None),
            P(None, "gx"),
            P("gx"),
            P("gx", None),
            P("gy", None, None),
            P("gy", "gx"),
            P("gx"),
            P("gx", "gy"),
        ),
        out_specs=(P("gy", "gx", None), P("gy", "gx")),
        check_vma=False,
    )
```

```python
import jax
import jax.numpy as jnp
from jax import lax
from jax.sharding import PartitionSpec as P

TSTEPS = 1000
BF = jnp.bfloat16
F32 = jnp.float32


def layer_norm(values):
    center = values - jnp.mean(values, axis=-1, keepdims=True)
    spread = jnp.mean(center * center, axis=-1, keepdims=True)
    return center * lax.rsqrt(spread + 1e-06)


def halves(block):
    cut = block.shape[0] // 2
    return [block[:cut], block[cut:]]


def add(a, b):
    return a.astype(F32) + b.astype(F32)


def flip(value, bit):
    n = lax.axis_size("gy")
    return lax.ppermute(value, "gy", [(i, i ^ bit) for i in range(n)])


def route(k):
    return k & -k, 1 << (k.bit_length() - 1)


def chip_offsets(n):
    return sorted(range(2, n, 2), key=lambda k: (bin(k).count("1"), k))


def plane_gather(own):
    n = lax.axis_size("gy")
    blocks = {0: own}
    for k in chip_offsets(n):
        blocks[k] = flip(own, k)
    for k in range(0, n, 2):
        blocks[k + 1] = flip(blocks[k], 1)
    return blocks


def plane_scatter(parts):
    n = lax.axis_size("gy")
    held = {k: halves(add(parts[k], flip(parts[k + 1], 1))) for k in range(0, n, 2)}
    for k in reversed(chip_offsets(n)):
        low, high = route(k)
        for half, bit in ((0, low), (1, high)):
            got = flip(held[k][half].astype(BF), bit)
            held[k ^ bit][half] = held[k ^ bit][half] + got.astype(F32)
    return jnp.concatenate(held[0], axis=0)


def shards(
    x_gen,
    fresh_noise,
    steps_t,
    real_mod,
    real_w_up,
    real_b_up,
    real_w_down,
    fake_mod,
    fake_w_up,
    fake_b_up,
    fake_w_down,
):
    n_gx, n_gy = lax.axis_size("gx"), lax.axis_size("gy")
    me = lax.axis_index("gy")
    noise_level = (steps_t[0].astype(F32) + 1.0) / TSTEPS
    clean_f = x_gen[0].astype(F32)
    drawn_f = fresh_noise[0].astype(F32)
    noised = ((1.0 - noise_level) * clean_f + noise_level * drawn_f).astype(BF)
    target = (drawn_f - clean_f).astype(BF)
    own_rows = noised.shape[0]
    wide = fake_w_up.shape[0]

    up_blocks = plane_gather(fake_w_up)
    noised_all = lax.all_gather(noised, "gx", axis=0, tiled=True)
    down_blocks = plane_gather(fake_w_down)

    def scatter_rows(part):
        rows = lax.psum_scatter(part, "gx", scatter_dimension=0, tiled=True)
        return rows.astype(F32)

    def columns(array, k):
        return lax.dynamic_slice_in_dim(array, (me ^ k) * wide, wide, axis=1)

    normed = layer_norm(noised_all.astype(F32))
    real_in = (normed * (1.0 + real_mod[0, 1]) + real_mod[0, 0]).astype(BF)
    fake_in = (normed * (1.0 + fake_mod[0, 1]) + fake_mod[0, 0]).astype(BF)
    real_in, fake_in = lax.optimization_barrier((real_in, fake_in))
    real_hidden = jax.nn.gelu(
        jnp.dot(real_in, real_w_up, preferred_element_type=F32) + real_b_up, approximate=True
    ).astype(BF)
    real_part = jnp.dot(real_hidden, real_w_down, preferred_element_type=F32).astype(BF)
    real_rows = scatter_rows(real_part)

    fake_pre = fake_b_up[None]
    for k in range(n_gy):
        fake_pre = fake_pre + jnp.dot(
            columns(fake_in, k), up_blocks[k], preferred_element_type=F32
        )
    fake_hidden = jax.nn.gelu(fake_pre, approximate=True).astype(BF)

    loss_scale = float(n_gy * n_gx * own_rows) ** (-0.5)
    products = {}
    group = max(2, n_gy // 2)
    chunks = [range(k, k + group) for k in range(n_gy - group, -1, -group)]
    preds = []
    for chunk in chunks:
        part = jnp.concatenate(
            [
                jnp.dot(fake_hidden, down_blocks[k], preferred_element_type=F32).astype(BF)
                for k in chunk
            ],
            axis=1,
        )
        preds.append(scatter_rows(part))
    for chunk, pred in zip(chunks, preds):
        goal = jnp.concatenate([columns(target, k) for k in chunk], axis=1)
        error = (pred - goal.astype(F32)).astype(BF)
        error_all = lax.all_gather(error, "gx", axis=0, tiled=True)
        for i, k in enumerate(chunk):
            part = slice(i * wide, (i + 1) * wide)
            product = lax.dot_general(
                error_all[:, part],
                fake_hidden,
                (((0,), (0,)), ((), ())),
                preferred_element_type=F32,
            )
            products[k] = (product * loss_scale).astype(BF)
    fake_grad = plane_scatter(products)
    relative = jnp.concatenate(preds[::-1], axis=1)
    fake_rows = jnp.concatenate([columns(relative, k) for k in range(n_gy)], axis=1)
    return ((fake_rows - real_rows)[None], fake_grad)


def solution(mesh):
    return jax.shard_map(
        shards,
        mesh=mesh,
        in_specs=(
            P("gy", "gx", None),
            P("gy", "gx", None),
            P("gy"),
            P("gy", None, None),
            P(None, "gx"),
            P("gx"),
            P("gx", None),
            P("gy", None, None),
            P("gy", "gx"),
            P("gx"),
            P("gx", "gy"),
        ),
        out_specs=(P("gy", "gx", None), P("gy", "gx")),
        check_vma=False,
    )
```
